32 devices in a mesh: dp: 8 (over y, x, core), mp: 4 (over z).
Axes of the slice: x: 2, y: 2, z: 4, core: 2. Of those that a mesh axis runs over, the one named last changes fastest.
Arguments:
- tokens: bfloat16 [512, 8192], P('mp', 'dp'), may hold values from -6 to 6
- cotangent: bfloat16 [512, 8192], P('mp', 'dp'), may hold values from -1.5 to 1.5
- gate_weight: bfloat16 [8192, 14336], P('dp', 'mp'), may hold values from -0.0625 to 0.0625
- up_weight: bfloat16 [8192, 14336], P('dp', 'mp'), may hold values from -0.0625 to 0.0625
- down_weight: bfloat16 [14336, 8192], P('mp', 'dp'), may hold values from -0.046875 to 0.046875
Outputs:
- output: bfloat16 [512, 8192], P('mp', 'dp')
- grad_input: bfloat16 [512, 8192], P('mp', 'dp')
- grad_gate: bfloat16 [8192, 14336], P('dp', 'mp')
- grad_up: bfloat16 [8192, 14336], P('dp', 'mp')
- grad_down: bfloat16 [14336, 8192], P('mp', 'dp')
The draws below stay inside these ranges and needn't reach their ends.
All inputs are finite; a program needn't handle non-finite values.
Results may differ from the reference program's by a relative error of at most 0.013.
Values may be sent and summed in bfloat16 or wider, within the bound.
A program may use at most 128 MiB of HBM per device.

```python
import jax
import jax.numpy as jnp
from jax import lax

D = 8192
FF = 14336
TOKENS = 512


def shard_levels(rng, extent, split, least, high):
    def one(position, blocks):
        steps = jax.random.uniform(jax.random.fold_in(jax.random.fold_in(rng, 6), position), (blocks,), jnp.float32, least / len(split), high / len(split))
        return jnp.repeat(jnp.exp(steps), extent[position] // blocks).reshape((-1,) + (1,) * (len(extent) - position - 1))

    factor_of = one(*split[0])
    for cut in split[1:]:
        factor_of = factor_of * one(*cut)
    return factor_of


def centred(key, shape, width, reach, shards=(), dtype=jnp.bfloat16):
    level = shard_levels(key, shape, shards, -0.22, 0.18) if shards else 1.0
    drawn = jax.random.normal(key, shape, jnp.float32) * width * level
    return jnp.minimum(jnp.maximum(drawn, -reach), reach).astype(dtype)


def setup_inputs(seed: int = 0) -> dict:
    splits = jax.random.split(jax.random.key(seed), 6)
    return {
        "tokens": centred(splits[0], (TOKENS, D), 1.0, 6.0, ((0, 4), (1, 8))),
        "cotangent": centred(splits[1], (TOKENS, D), 0.25, 1.5, ((0, 4), (1, 8))),
        "gate_weight": centred(splits[2], (D, FF), D ** -0.5, 0.0625, ((0, 8), (1, 4))),
        "up_weight": centred(splits[3], (D, FF), D ** -0.5, 0.0625, ((0, 8), (1, 4))),
        "down_weight": centred(splits[4], (FF, D), FF ** -0.5, 0.046875, ((0, 4), (1, 8))),
    }


def contract(left, right, left_dim, right_dim):
    return lax.dot_general(left, right, (((left_dim,), (right_dim,)), ((), ())), preferred_element_type=jnp.float32)


def reference(tokens, cotangent, gate_weight, up_weight, down_weight):
    gate = jnp.dot(tokens, gate_weight, preferred_element_type=jnp.float32)
    up = jnp.dot(tokens, up_weight, preferred_element_type=jnp.float32)
    sig = jax.nn.sigmoid(gate)
    hidden = (gate * sig * up).astype(jnp.bfloat16)
    output = jnp.dot(hidden, down_weight, preferred_element_type=jnp.float32).astype(jnp.bfloat16)
    d_hidden = contract(cotangent, down_weight, 1, 1)
    d_gate = (d_hidden * up * sig * (1.0 + gate * (1.0 - sig))).astype(jnp.bfloat16)
    d_up = (d_hidden * gate * sig).astype(jnp.bfloat16)
    grad_down = contract(hidden, cotangent, 0, 0).astype(jnp.bfloat16)
    grad_gate = contract(tokens, d_gate, 0, 0).astype(jnp.bfloat16)
    grad_up = contract(tokens, d_up, 0, 0).astype(jnp.bfloat16)
    grad_input = (contract(d_gate, gate_weight, 1, 1) + contract(d_up, up_weight, 1, 1)).astype(jnp.bfloat16)
    return (output, grad_input, grad_gate, grad_up, grad_down)
```

```python
import functools

import jax
import jax.numpy as jnp
from jax import lax
from jax.experimental import pallas as pl
from jax.experimental.pallas import tpu as pltpu
from jax.sharding import PartitionSpec as P

F32, BF16 = jnp.float32, jnp.bfloat16
MESH = pl.DeviceIdType.MESH

HALVES = 2
ORDER = (
    ("gate", 0), ("rs2", 1), ("up", 0), ("rs3", 2), ("down", 0),
    ("ag2", 3), ("rs1", 0), ("ag1", 4), ("ag0", 5),
)


def contract(left, right, left_dim, right_dim):
    return lax.dot_general(
        left, right, (((left_dim,), (right_dim,)), ((), ())), preferred_element_type=F32
    )


def tasks_of(bits):
    if bits == 3:
        return ORDER
    order = [("gate", 0), ("up", 0), ("down", 0), ("rs1", 0)]
    order += [(f"rs{r}", r - 1) for r in range(2, bits + 1)]
    order += [(f"ag{a}", 2 * bits - 1 - a) for a in range(bits - 1, -1, -1)]
    return tuple(order)


def mixer(
    n_dp, n_mp, halves,
    x_in, c_in, wg_in, wu_in, wd_in,
    out_ref, gin_ref, ax_ref, ac_ref, hid_out, dg_out, du_out,
    xs, cs, wg, wu, wd, hid, dg, du, psum, acc, osend, orecv, *rest,
):
    bits = n_dp.bit_length() - 1
    snd, rcv, kept = rest[:bits], rest[bits:2 * bits], rest[2 * bits:3 * bits - 1]
    (rs_send, rs_recv, ag_send, ag_recv, w_sem, own_sem, tz_send, tz_recv,
     o_send, o_recv, act_sem, grid_sem) = rest[3 * bits - 1:]
    units = n_mp * halves
    pieces, rows, cols = psum.shape[1:]
    tall = pieces * rows
    gathered = (hid, dg, du)

    me, z = lax.axis_index("dp"), lax.axis_index("mp")
    parity = me % 2
    even = [0] + list(range(1, bits))
    odd = [0] + list(range(bits - 1, 0, -1))
    partner, offset, mine = [], [0], []
    for s in range(bits):
        width = (1 << even[s]) * (1 - parity) + (1 << odd[s]) * parity
        bit = (me // width) % 2
        mine.append(bit)
        partner.append(me + width * (1 - 2 * bit))
        offset.append(offset[-1] + bit * (pieces >> (s + 1)))

    barrier = pltpu.get_barrier_semaphore()
    for s in range(bits):
        pl.semaphore_signal(barrier, inc=1, device_id={"dp": partner[s]}, device_id_type=MESH)
    for k in range(1, n_mp):
        pl.semaphore_signal(barrier, inc=1, device_id={"mp": (z + k) % n_mp}, device_id_type=MESH)

    own = [
        pltpu.make_async_copy(x_in, xs.at[z], own_sem.at[0]),
        pltpu.make_async_copy(c_in, cs.at[z], own_sem.at[1]),
    ]

    def weight(which, h):
        place = pl.ds(pl.multiple_of(h * cols, 128), cols)
        source = (wg_in.at[:, place], wu_in.at[:, place], wd_in.at[place, :])[which]
        return pltpu.make_async_copy(source, (wg, wu, wd)[which].at[h], w_sem.at[which, h])

    own[0].start()
    weight(0, halves - 1).start()
    own[1].start()
    weight(1, halves - 1).start()
    weight(2, halves - 1).start()
    for h in range(halves - 1):
        for which in range(3):
            weight(which, h).start()

    pl.semaphore_wait(barrier, bits + n_mp - 1)

    def spread(which, k):
        buf = (xs, cs)[which]
        return pltpu.make_async_remote_copy(
            src_ref=buf.at[z], dst_ref=buf.at[z],
            send_sem=tz_send.at[which, k - 1], recv_sem=tz_recv.at[which, k - 1],
            device_id={"mp": (z - k + n_mp) % n_mp}, device_id_type=MESH,
        )

    own[0].wait()
    if n_mp > 1:
        spread(0, 1).start()
    own[1].wait()
    if n_mp > 1:
        spread(1, 1).start()
    for k in range(2, n_mp):
        for which in range(2):
            spread(which, k).start()

    def arrived(which, k):
        buf = (xs, cs)[which]
        src = (z + k) % n_mp
        pltpu.make_async_remote_copy(
            src_ref=buf.at[src], dst_ref=buf.at[src],
            send_sem=tz_send.at[which, k - 1], recv_sem=tz_recv.at[which, k - 1],
            device_id={"mp": src}, device_id_type=MESH,
        ).wait_recv()

    def place_of(u):
        k = ((u + halves - 1) // halves) % n_mp
        h = (u + halves - 1) % halves
        return k, h, (z + k) % n_mp

    def keep_out(which, zz):
        return pltpu.make_async_copy(
            (xs, cs)[which].at[zz], (ax_ref, ac_ref)[which].at[zz], grid_sem.at[which, zz]
        )

    def put_out(i, h, zz, u):
        return pltpu.make_async_copy(
            gathered[i].at[zz, h],
            (hid_out, dg_out, du_out)[i].at[zz, :, :, pl.ds(pl.multiple_of(h * cols, 128), cols)],
            act_sem.at[u, i],
        )

    def rs(s, u, i):
        return pltpu.make_async_remote_copy(
            src_ref=snd[s].at[u % 2, i], dst_ref=rcv[s].at[u, i],
            send_sem=rs_send.at[s, u % 2, i], recv_sem=rs_recv.at[s, u, i],
            device_id={"dp": partner[s]}, device_id_type=MESH,
        )

    def ag(s, u, i, arriving=False):
        k, h, zz = place_of(u)
        size = pieces >> (s + 1)
        start = offset[s] + (1 - mine[s]) * size if arriving else offset[s + 1]
        there = gathered[i].at[zz, h, pl.ds(start, size)]
        return pltpu.make_async_remote_copy(
            src_ref=there, dst_ref=there,
            send_sem=ag_send.at[s, u % 2, i], recv_sem=ag_recv.at[s, u, i],
            device_id={"dp": partner[s]}, device_id_type=MESH,
        )

    def forward(i, u):
        k, h, zz = place_of(u)
        which = (0, 0, 1)[i]
        if i != 1:
            for kk in range(1, n_mp):
                @pl.when((k == kk) & (h == 0))
                def _():
                    arrived(which, kk)

        @pl.when(u < halves)
        def _():
            weight(i, h).wait()

        if i == 0:
            total = contract(xs[zz], wg[h], 1, 0)
        elif i == 1:
            total = contract(xs[zz], wu[h], 1, 0)
        else:
            total = contract(cs[zz], wd[h], 1, 1)
        psum[i] = total.reshape(pieces, rows, cols)

        @pl.when(u >= 2)
        def _():
            rs(0, u - 2, i).wait_send()

        half = pieces // 2
        snd[0][u % 2, i] = psum[i, pl.ds((1 - mine[0]) * half, half)].astype(BF16)
        rs(0, u, i).start()

    def reduce(r, u):
        size = pieces >> r
        for i in range(3):
            rs(r - 1, u, i).wait_recv()
            if r == 1:
                old = psum.at[i, pl.ds(mine[0] * size, size)]
            else:
                old = kept[r - 2].at[u % 2, i]
            half = size // 2
            away, stay = (1 - mine[r]) * half, mine[r] * half

            @pl.when(u >= 2)
            def _():
                rs(r, u - 2, i).wait_send()

            new = rcv[r - 1].at[u, i]
            snd[r][u % 2, i] = (old[pl.ds(away, half)] + new[pl.ds(away, half)].astype(F32)).astype(BF16)
            rs(r, u, i).start()
            kept[r - 1][u % 2, i] = old[pl.ds(stay, half)] + new[pl.ds(stay, half)].astype(F32)

    def finish(u):
        k, h, zz = place_of(u)
        sums = []
        for i in range(3):
            rs(bits - 1, u, i).wait_recv()
            last = kept[bits - 2][u % 2, i] if bits > 1 else psum[i, pl.ds(mine[0], 1)]
            sums.append(last + rcv[bits - 1][u, i].astype(F32))
        gate, up, d_hidden = sums
        sig = 1.0 / (1.0 + jnp.exp(-gate))
        at = pl.ds(offset[bits], 1)
        hid[zz, h, at] = (gate * sig * up).astype(BF16)
        dg[zz, h, at] = (d_hidden * up * sig * (1.0 + gate * (1.0 - sig))).astype(BF16)
        du[zz, h, at] = (d_hidden * gate * sig).astype(BF16)
        for i in range(3):
            @pl.when(u >= 2)
            def _():
                ag(bits - 1, u - 2, i).wait_send()
            ag(bits - 1, u, i).start()

    def widen(a, u):
        for i in range(3):
            ag(a, u, i, arriving=True).wait_recv()

            @pl.when(u >= 2)
            def _():
                ag(a - 1, u - 2, i).wait_send()
            ag(a - 1, u, i).start()

    def backward(u):
        k, h, zz = place_of(u)
        other = jnp.minimum(k, 1)

        @pl.when((u == 0) | ((k > 0) & (h == 0)))
        def _():
            acc[other] = jnp.zeros(acc.shape[1:], F32)

        for i in range(3):
            ag(0, u, i, arriving=True).wait_recv()
            put_out(i, h, zz, u).start()
            left = gathered[i][zz, h].reshape(tall, cols)
            if i == 0:
                acc[other, 0] += contract(left, wd[h], 1, 0)
            elif i == 1:
                acc[other, 1] += contract(left, wg[h], 1, 1)
            else:
                acc[other, 1] += contract(left, wu[h], 1, 1)

        @pl.when((k > 0) & (h == halves - 1))
        def _():
            for i in range(2):
                osend[k - 1, i] = acc[1, i].astype(BF16)
                partial(i, k).start()

    def partial(i, k):
        return pltpu.make_async_remote_copy(
            src_ref=osend.at[k - 1, i], dst_ref=orecv.at[k - 1, i],
            send_sem=o_send.at[k - 1, i], recv_sem=o_recv.at[k - 1, i],
            device_id={"mp": (z + k) % n_mp}, device_id_type=MESH,
        )

    run = {"gate": functools.partial(forward, 0), "up": functools.partial(forward, 1),
           "down": functools.partial(forward, 2)}
    for r in range(1, bits):
        run[f"rs{r}"] = functools.partial(reduce, r)
        run[f"ag{r}"] = functools.partial(widen, r)
    run[f"rs{bits}"] = finish
    run["ag0"] = backward
    order = tasks_of(bits)
    depth = max(lag for _, lag in order)

    def step(t, carry):
        for name, lag in order:
            u = t - lag

            @pl.when((u >= 0) & (u < units))
            def _():
                run[name](u)
        return carry

    lax.fori_loop(0, units + depth, step, 0)

    for zz in range(n_mp):
        for which in range(2):
            keep_out(which, zz).start()
    for i in range(2):
        total = acc[0, i]
        for k in range(1, n_mp):
            partial(i, k).wait_recv()
            total += orecv[k - 1, i].astype(F32)
        (out_ref, gin_ref)[i][...] = total.astype(BF16)

    for k in range(1, n_mp):
        for i in range(2):
            spread(i, k).wait_send()
            partial(i, k).wait_send()
    first = max(units - 2, 0)
    for u in range(first, units):
        for s in range(bits):
            for i in range(3):
                rs(s, u, i).wait_send()
                ag(s, u, i).wait_send()

    def drain(u, carry):
        k, h, zz = place_of(u)
        for i in range(3):
            put_out(i, h, zz, u).wait()
        return carry

    lax.fori_loop(0, units, drain, 0)
    for zz in range(n_mp):
        for which in range(2):
            keep_out(which, zz).wait()


def per_device(tokens, cotangent, gate_weight, up_weight, down_weight):
    n_dp, n_mp = lax.axis_size("dp"), lax.axis_size("mp")
    bits = n_dp.bit_length() - 1
    assert 1 << bits == n_dp and bits >= 2
    tall, width = tokens.shape
    inner = gate_weight.shape[1]
    halves = HALVES
    cols, units = inner // halves, n_mp * halves
    rows = tall // n_dp
    assert rows * n_dp == tall and cols * halves == inner

    vmem, any_ = pltpu.VMEM, pl.BlockSpec(memory_space=pl.ANY)
    in_vmem = pl.BlockSpec(memory_space=pltpu.VMEM)
    sizes = [n_dp >> (s + 1) for s in range(bits)]
    dma = pltpu.SemaphoreType.DMA
    scratch = [
        vmem((n_mp, tall, width), BF16), vmem((n_mp, tall, width), BF16),
        vmem((halves, width, cols), BF16), vmem((halves, width, cols), BF16),
        vmem((halves, cols, width), BF16),
    ]
    scratch += [vmem((n_mp, halves, n_dp, rows, cols), BF16)] * 3
    scratch += [
        vmem((3, n_dp, rows, cols), F32), vmem((2, 2, tall, width), F32),
        vmem((n_mp - 1, 2, tall, width), BF16), vmem((n_mp - 1, 2, tall, width), BF16),
    ]
    scratch += [vmem((2, 3, size, rows, cols), BF16) for size in sizes]
    scratch += [vmem((units, 3, size, rows, cols), BF16) for size in sizes]
    scratch += [vmem((2, 3, size, rows, cols), F32) for size in sizes[1:]]
    scratch += [
        dma((bits, 2, 3)), dma((bits, units, 3)), dma((bits, 2, 3)), dma((bits, units, 3)),
        dma((3, halves)), dma((2,)), dma((2, n_mp - 1)), dma((2, n_mp - 1)),
        dma((n_mp - 1, 2)), dma((n_mp - 1, 2)), dma((units, 3)), dma((2, n_mp)),
    ]
    small = jax.ShapeDtypeStruct((tall, width), BF16)
    all_rows = jax.ShapeDtypeStruct((n_mp, tall, width), BF16)
    active = jax.ShapeDtypeStruct((n_mp, n_dp, rows, inner), BF16)
    output, grad_input, all_x, all_c, hidden, d_gate, d_up = pl.pallas_call(
        functools.partial(mixer, n_dp, n_mp, halves),
        out_shape=(small, small, all_rows, all_rows, active, active, active),
        in_specs=[any_] * 5,
        out_specs=(in_vmem, in_vmem) + (any_,) * 5,
        scratch_shapes=scratch,
        compiler_params=pltpu.CompilerParams(
            collective_id=0, has_side_effects=True, vmem_limit_bytes=67043328
        ),
    )(tokens, cotangent, gate_weight, up_weight, down_weight)

    whole = n_mp * tall
    all_x, all_c = all_x.reshape(whole, width), all_c.reshape(whole, width)
    hidden, d_gate, d_up = (a.reshape(whole, inner) for a in (hidden, d_gate, d_up))
    turned = all_x.T
    grad_down = contract(hidden, all_c, 0, 0).astype(BF16)
    grad_gate = contract(turned, d_gate, 1, 0).astype(BF16)
    grad_up = contract(turned, d_up, 1, 0).astype(BF16)
    return (output, grad_input, grad_gate, grad_up, grad_down)


def solution(mesh):
    placed = (P("mp", "dp"), P("mp", "dp"), P("dp", "mp"), P("dp", "mp"), P("mp", "dp"))
    return jax.shard_map(
        per_device,
        mesh=mesh,
        in_specs=placed,
        out_specs=(P("mp", "dp"), P("mp", "dp"), P("dp", "mp"), P("dp", "mp"), P("mp", "dp")),
        check_vma=False,
    )
```

```python
import functools

import jax
import jax.numpy as jnp
from jax import lax
from jax.experimental import pallas as pl
from jax.experimental.pallas import tpu as pltpu
from jax.sharding import PartitionSpec as P

F32, BF16 = jnp.float32, jnp.bfloat16
MESH = pl.DeviceIdType.MESH

HALVES = 2
ORDER = (
    ("gate", 0),
    ("up", 0),
    ("down", 0),
    ("rs1", 0),
    ("rs2", 1),
    ("rs3", 2),
    ("ag2", 3),
    ("ag1", 4),
    ("ag0", 4),
)


def contract(left, right, left_dim, right_dim):
    return lax.dot_general(
        left, right, (((left_dim,), (right_dim,)), ((), ())), preferred_element_type=F32
    )


def tasks_of(bits):
    if bits == 3:
        return ORDER
    order = [("gate", 0), ("up", 0), ("down", 0), ("rs1", 0)]
    order += [(f"rs{r}", r - 1) for r in range(2, bits + 1)]
    order += [(f"ag{a}", 2 * bits - 1 - a) for a in range(bits - 1, -1, -1)]
    return tuple(order)


def mixer(
    n_dp, n_mp, halves,
    x_in, c_in, wg_in, wu_in, wd_in,
    mine_ref, last_ref, ax_ref, ac_ref, hid_out, dg_out, du_out,
    xs, cs, wg, wu, wd, hid, dg, du, psum, acc, osend, orecv, *rest,
):
    bits = n_dp.bit_length() - 1
    snd, rcv, kept = rest[:bits], rest[bits:2 * bits], rest[2 * bits:3 * bits - 1]
    (rs_send, rs_recv, ag_send, ag_recv, w_sem, own_sem, tz_send, tz_recv,
     o_send, o_recv, act_sem, grid_sem) = rest[3 * bits - 1:]
    units = n_mp * halves
    pieces, rows, cols = psum.shape[1:]
    tall = pieces * rows
    gathered = (hid, dg, du)

    me, z = lax.axis_index("dp"), lax.axis_index("mp")
    parity = me % 2
    even = [0] + list(range(1, bits))
    odd = [0] + list(range(bits - 1, 0, -1))
    partner, offset, mine = [], [0], []
    for s in range(bits):
        width = (1 << even[s]) * (1 - parity) + (1 << odd[s]) * parity
        bit = (me // width) % 2
        mine.append(bit)
        partner.append(me + width * (1 - 2 * bit))
        offset.append(offset[-1] + bit * (pieces >> (s + 1)))

    barrier = pltpu.get_barrier_semaphore()
    for s in range(bits):
        pl.semaphore_signal(barrier, inc=1, device_id={"dp": partner[s]}, device_id_type=MESH)
    for k in (1, n_mp - 1):
        pl.semaphore_signal(barrier, inc=1, device_id={"mp": (z + k) % n_mp}, device_id_type=MESH)

    own = [
        pltpu.make_async_copy(x_in, xs.at[z], own_sem.at[0]),
        pltpu.make_async_copy(c_in, cs.at[z], own_sem.at[1]),
    ]

    def weight(which, h):
        place = pl.ds(pl.multiple_of(h * cols, 128), cols)
        source = (wg_in.at[:, place], wu_in.at[:, place], wd_in.at[place, :])[which]
        return pltpu.make_async_copy(source, (wg, wu, wd)[which].at[h], w_sem.at[which, h])

    own[0].start()
    weight(0, 0).start()
    own[1].start()
    weight(1, 0).start()
    weight(2, 0).start()
    for h in range(1, halves):
        for which in range(3):
            weight(which, h).start()

    pl.semaphore_wait(barrier, bits + 2)

    below = {"mp": (z + n_mp - 1) % n_mp}

    def spread(which, p):
        there = (xs, cs)[which].at[(z + p - 1) % n_mp]
        return pltpu.make_async_remote_copy(
            src_ref=there, dst_ref=there,
            send_sem=tz_send.at[which, p - 1], recv_sem=tz_recv.at[which, p - 1],
            device_id=below, device_id_type=MESH,
        )

    def arrived(which, p):
        there = (xs, cs)[which].at[(z + p) % n_mp]
        return pltpu.make_async_remote_copy(
            src_ref=there, dst_ref=there,
            send_sem=tz_send.at[which, p - 1], recv_sem=tz_recv.at[which, p - 1],
            device_id=below, device_id_type=MESH,
        )

    for which in range(2):
        own[which].wait()
        spread(which, 1).start()

    def place_of(u):
        k = u // halves
        return k, u % halves, (z + k) % n_mp

    def keep_out(which, zz):
        return pltpu.make_async_copy(
            (xs, cs)[which].at[zz], (ax_ref, ac_ref)[which].at[zz], grid_sem.at[which, zz]
        )

    def put_out(i, h, zz, u):
        return pltpu.make_async_copy(
            gathered[i].at[zz, h],
            (hid_out, dg_out, du_out)[i].at[zz, :, :, pl.ds(pl.multiple_of(h * cols, 128), cols)],
            act_sem.at[u, i],
        )

    def rs(s, u, i):
        return pltpu.make_async_remote_copy(
            src_ref=snd[s].at[u % 2, i], dst_ref=rcv[s].at[u, i],
            send_sem=rs_send.at[s, u % 2, i], recv_sem=rs_recv.at[s, u, i],
            device_id={"dp": partner[s]}, device_id_type=MESH,
        )

    def ag(s, u, i, arriving=False):
        k, h, zz = place_of(u)
        size = pieces >> (s + 1)
        start = offset[s] + (1 - mine[s]) * size if arriving else offset[s + 1]
        there = gathered[i].at[zz, h, pl.ds(start, size)]
        return pltpu.make_async_remote_copy(
            src_ref=there, dst_ref=there,
            send_sem=ag_send.at[s, u % 2, i], recv_sem=ag_recv.at[s, u, i],
            device_id={"dp": partner[s]}, device_id_type=MESH,
        )

    def forward(i, u):
        k, h, zz = place_of(u)
        which = (0, 0, 1)[i]
        if i != 1:
            @pl.when((k > 0) & (h == 0))
            def _():
                arrived(which, k).wait_recv()

                @pl.when(k < n_mp - 1)
                def _():
                    spread(which, k + 1).start()

            @pl.when(h == 0)
            def _():
                keep_out(which, zz).start()

        @pl.when(u < halves)
        def _():
            weight(i, h).wait()

        if i == 0:
            total = contract(xs[zz], wg[h], 1, 0)
        elif i == 1:
            total = contract(xs[zz], wu[h], 1, 0)
        else:
            total = contract(cs[zz], wd[h], 1, 1)
        psum[i] = total.reshape(pieces, rows, cols)

        @pl.when(u >= 2)
        def _():
            rs(0, u - 2, i).wait_send()

        half = pieces // 2
        snd[0][u % 2, i] = psum[i, pl.ds((1 - mine[0]) * half, half)].astype(BF16)
        rs(0, u, i).start()

    def reduce(r, u):
        size = pieces >> r
        for i in range(3):
            rs(r - 1, u, i).wait_recv()
            if r == 1:
                old = psum.at[i, pl.ds(mine[0] * size, size)]
            else:
                old = kept[r - 2].at[u % 2, i]
            half = size // 2
            away, stay = (1 - mine[r]) * half, mine[r] * half

            @pl.when(u >= 2)
            def _():
                rs(r, u - 2, i).wait_send()

            new = rcv[r - 1].at[u, i]
            snd[r][u % 2, i] = (old[pl.ds(away, half)] + new[pl.ds(away, half)].astype(F32)).astype(BF16)
            rs(r, u, i).start()
            kept[r - 1][u % 2, i] = old[pl.ds(stay, half)] + new[pl.ds(stay, half)].astype(F32)

    def finish(u):
        k, h, zz = place_of(u)
        sums = []
        for i in range(3):
            rs(bits - 1, u, i).wait_recv()
            last = kept[bits - 2][u % 2, i] if bits > 1 else psum[i, pl.ds(mine[0], 1)]
            sums.append(last + rcv[bits - 1][u, i].astype(F32))
        gate, up, d_hidden = sums
        sig = 1.0 / (1.0 + jnp.exp(-gate))
        at = pl.ds(offset[bits], 1)
        hid[zz, h, at] = (gate * sig * up).astype(BF16)
        dg[zz, h, at] = (d_hidden * up * sig * (1.0 + gate * (1.0 - sig))).astype(BF16)
        du[zz, h, at] = (d_hidden * gate * sig).astype(BF16)
        for i in range(3):
            @pl.when(u >= 2)
            def _():
                ag(bits - 1, u - 2, i).wait_send()
            ag(bits - 1, u, i).start()

    def widen(a, u):
        for i in range(3):
            ag(a, u, i, arriving=True).wait_recv()

            @pl.when(u >= 2)
            def _():
                ag(a - 1, u - 2, i).wait_send()
            ag(a - 1, u, i).start()

    def backward(u):
        k, h, zz = place_of(u)
        other = jnp.minimum(k, 1)

        @pl.when(h == 0)
        def _():
            acc[other] = jnp.zeros(acc.shape[1:], F32)

        for i in range(3):
            ag(0, u, i, arriving=True).wait_recv()
            put_out(i, h, zz, u).start()
            left = gathered[i][zz, h].reshape(tall, cols)
            if i == 0:
                acc[other, 0] += contract(left, wd[h], 1, 0)
            elif i == 1:
                acc[other, 1] += contract(left, wg[h], 1, 1)
            else:
                acc[other, 1] += contract(left, wu[h], 1, 1)

        @pl.when((k > 0) & (k < n_mp - 1) & (h == halves - 1))
        def _():
            for i in range(2):
                total = passed(i, k)
                osend[k - 1, i] = total.astype(BF16)
                partial(i, k).start()

    def partial(i, k):
        return pltpu.make_async_remote_copy(
            src_ref=osend.at[k - 1, i], dst_ref=orecv.at[k, i],
            send_sem=o_send.at[k - 1, i], recv_sem=o_recv.at[k - 1, i],
            device_id=below, device_id_type=MESH,
        )

    def passed(i, k):
        @pl.when(k > 1)
        def _():
            partial(i, k - 1).wait_recv()
        return acc[1, i] + orecv[k - 1, i].astype(F32)

    run = {"gate": functools.partial(forward, 0), "up": functools.partial(forward, 1),
           "down": functools.partial(forward, 2)}
    for r in range(1, bits):
        run[f"rs{r}"] = functools.partial(reduce, r)
        run[f"ag{r}"] = functools.partial(widen, r)
    run[f"rs{bits}"] = finish
    run["ag0"] = backward
    orecv[0] = jnp.zeros(orecv.shape[1:], BF16)
    order = tasks_of(bits)
    depth = max(lag for _, lag in order)

    def step(t, carry):
        for name, lag in order:
            u = t - lag

            @pl.when((u >= 0) & (u < units))
            def _():
                run[name](u)
        return carry

    lax.fori_loop(0, units + depth, step, 0)

    for i in range(2):
        last_ref[i] = passed(i, n_mp - 1).astype(BF16)
        mine_ref[i] = acc[0, i]

    for p in range(1, n_mp):
        for i in range(2):
            spread(i, p).wait_send()
            if p < n_mp - 1:
                partial(i, p).wait_send()
    first = max(units - 2, 0)
    for u in range(first, units):
        for s in range(bits):
            for i in range(3):
                rs(s, u, i).wait_send()
                ag(s, u, i).wait_send()

    def drain(u, carry):
        k, h, zz = place_of(u)
        for i in range(3):
            put_out(i, h, zz, u).wait()
        return carry

    lax.fori_loop(0, units, drain, 0)
    for zz in range(n_mp):
        for which in range(2):
            keep_out(which, zz).wait()


def gradients(x_ref, c_ref, h_ref, g_ref, u_ref, gg_ref, gu_ref, gd_ref, turned):
    @pl.when(pl.program_id(0) == 0)
    def _():
        turned[...] = x_ref[...].T

    gd_ref[...] = contract(h_ref[...], c_ref[...], 0, 0).astype(BF16)
    gg_ref[...] = contract(turned[...], g_ref[...], 1, 0).astype(BF16)
    gu_ref[...] = contract(turned[...], u_ref[...], 1, 0).astype(BF16)


def weight_gradients(x, c, hidden, d_gate, d_up):
    (tall, width), inner = x.shape, hidden.shape[1]
    tile = next(t for t in (512, 256, 128) if inner % t == 0)
    fixed = pl.BlockSpec((tall, width), lambda i: (0, 0), pipeline_mode=pl.Buffered(1))
    active = pl.BlockSpec((tall, tile), lambda i: (0, i))
    wide = pl.BlockSpec((width, tile), lambda i: (0, i))
    deep = pl.BlockSpec((tile, width), lambda i: (i, 0))
    return pl.pallas_call(
        gradients,
        grid=(inner // tile,),
        out_shape=(
            jax.ShapeDtypeStruct((width, inner), BF16), jax.ShapeDtypeStruct((width, inner), BF16),
            jax.ShapeDtypeStruct((inner, width), BF16),
        ),
        in_specs=[fixed, fixed, active, active, active],
        out_specs=(wide, wide, deep),
        scratch_shapes=[pltpu.VMEM((width, tall), BF16)],
        compiler_params=pltpu.CompilerParams(vmem_limit_bytes=60 << 20),
        cost_estimate=pl.CostEstimate(
            flops=6 * tall * width * inner, transcendentals=0,
            bytes_accessed=6 * (tall + width) * inner + 4 * tall * width,
        ),
    )(x, c, hidden, d_gate, d_up)


def per_device(tokens, cotangent, gate_weight, up_weight, down_weight):
    n_dp, n_mp = lax.axis_size("dp"), lax.axis_size("mp")
    bits = n_dp.bit_length() - 1
    assert 1 << bits == n_dp and bits >= 2 and n_mp >= 3
    tall, width = tokens.shape
    inner = gate_weight.shape[1]
    halves = HALVES
    cols, units = inner // halves, n_mp * halves
    rows = tall // n_dp
    assert rows * n_dp == tall and cols * halves == inner

    vmem, any_ = pltpu.VMEM, pl.BlockSpec(memory_space=pl.ANY)
    in_vmem = pl.BlockSpec(memory_space=pltpu.VMEM)
    sizes = [n_dp >> (s + 1) for s in range(bits)]
    dma = pltpu.SemaphoreType.DMA
    scratch = [
        vmem((n_mp, tall, width), BF16), vmem((n_mp, tall, width), BF16),
        vmem((halves, width, cols), BF16), vmem((halves, width, cols), BF16),
        vmem((halves, cols, width), BF16),
    ]
    scratch += [vmem((n_mp, halves, n_dp, rows, cols), BF16)] * 3
    scratch += [
        vmem((3, n_dp, rows, cols), F32), vmem((2, 2, tall, width), F32),
        vmem((n_mp - 2, 2, tall, width), BF16), vmem((n_mp - 1, 2, tall, width), BF16),
    ]
    scratch += [vmem((2, 3, size, rows, cols), BF16) for size in sizes]
    scratch += [vmem((units, 3, size, rows, cols), BF16) for size in sizes]
    scratch += [vmem((2, 3, size, rows, cols), F32) for size in sizes[1:]]
    scratch += [
        dma((bits, 2, 3)), dma((bits, units, 3)), dma((bits, 2, 3)), dma((bits, units, 3)),
        dma((3, halves)), dma((2,)), dma((2, n_mp - 1)), dma((2, n_mp - 1)),
        dma((n_mp - 2, 2)), dma((n_mp - 2, 2)), dma((units, 3)), dma((2, n_mp)),
    ]
    small = [jax.ShapeDtypeStruct((2, tall, width), dtype) for dtype in (F32, BF16)]
    all_rows = jax.ShapeDtypeStruct((n_mp, tall, width), BF16)
    active = jax.ShapeDtypeStruct((n_mp, n_dp, rows, inner), BF16)
    mine, last, all_x, all_c, hidden, d_gate, d_up = pl.pallas_call(
        functools.partial(mixer, n_dp, n_mp, halves),
        out_shape=(*small, all_rows, all_rows, active, active, active),
        in_specs=[any_] * 5,
        out_specs=(in_vmem, in_vmem) + (any_,) * 5,
        scratch_shapes=scratch,
        compiler_params=pltpu.CompilerParams(
            collective_id=0, has_side_effects=True, vmem_limit_bytes=67043328
        ),
    )(tokens, cotangent, gate_weight, up_weight, down_weight)

    whole = n_mp * tall
    all_x, all_c = all_x.reshape(whole, width), all_c.reshape(whole, width)
    hidden, d_gate, d_up = (a.reshape(whole, inner) for a in (hidden, d_gate, d_up))
    come = lax.ppermute(last, "mp", [(i, (i - 1) % n_mp) for i in range(n_mp)])
    grad_gate, grad_up, grad_down = weight_gradients(all_x, all_c, hidden, d_gate, d_up)
    output, grad_input = (mine + come.astype(F32)).astype(BF16)
    return (output, grad_input, grad_gate, grad_up, grad_down)


def solution(mesh):
    placed = (P("mp", "dp"), P("mp", "dp"), P("dp", "mp"), P("dp", "mp"), P("mp", "dp"))
    return jax.shard_map(
        per_device,
        mesh=mesh,
        in_specs=placed,
        out_specs=(P("mp", "dp"), P("mp", "dp"), P("dp", "mp"), P("dp", "mp"), P("mp", "dp")),
        check_vma=False,
    )
```

```python
import functools

import jax
import jax.numpy as jnp
from jax import lax
from jax.experimental import pallas as pl
from jax.experimental.pallas import tpu as pltpu
from jax.sharding import PartitionSpec as P

F32, BF16 = jnp.float32, jnp.bfloat16
MESH = pl.DeviceIdType.MESH

HALVES = 2
ORDER = (
    ("gate", 0),
    ("up", 0),
    ("rs1 gate", 0),
    ("down", 0),
    ("rs1 up", 0),
    ("rs1 down", 0),
    ("rs3", 2),
    ("rs2", 1),
    ("ag2", 3),
    ("ag1", 4),
    ("ag0", 4),
)


def contract(left, right, left_dim, right_dim):
    return lax.dot_general(
        left, right, (((left_dim,), (right_dim,)), ((), ())), preferred_element_type=F32
    )


def tasks_of(bits):
    if bits == 3:
        return ORDER
    order = [("gate", 0), ("up", 0), ("down", 0), ("rs1", 0)]
    order += [(f"rs{r}", r - 1) for r in range(2, bits + 1)]
    order += [(f"ag{a}", 2 * bits - 1 - a) for a in range(bits - 1, -1, -1)]
    return tuple(order)


def mixer(
    n_dp, n_mp, halves,
    x_in, c_in, wg_in, wu_in, wd_in,
    mine_ref, last_ref, ax_ref, ac_ref, hid_out, dg_out, du_out,
    xs, cs, wg, wu, wd, hid, dg, du, psum, acc, osend, orecv, *rest,
):
    bits = n_dp.bit_length() - 1
    snd, rcv, kept = rest[:bits], rest[bits:2 * bits], rest[2 * bits:3 * bits - 1]
    (rs_send, rs_recv, ag_send, ag_recv, w_sem, own_sem, tz_send, tz_recv,
     o_send, o_recv, act_sem, grid_sem) = rest[3 * bits - 1:]
    units = n_mp * halves
    pieces, rows, cols = psum.shape[1:]
    tall = pieces * rows
    gathered = (hid, dg, du)

    me, z = lax.axis_index("dp"), lax.axis_index("mp")
    parity = me % 2
    even = [0] + list(range(1, bits))
    odd = [0] + list(range(bits - 1, 0, -1))
    partner, offset, mine = [], [0], []
    for s in range(bits):
        width = (1 << even[s]) * (1 - parity) + (1 << odd[s]) * parity
        bit = (me // width) % 2
        mine.append(bit)
        partner.append(me + width * (1 - 2 * bit))
        offset.append(offset[-1] + bit * (pieces >> (s + 1)))

    barrier = pltpu.get_barrier_semaphore()
    for s in range(bits):
        pl.semaphore_signal(barrier, inc=1, device_id={"dp": partner[s]}, device_id_type=MESH)
    for k in (1, n_mp - 1):
        pl.semaphore_signal(barrier, inc=1, device_id={"mp": (z + k) % n_mp}, device_id_type=MESH)

    own = [
        pltpu.make_async_copy(x_in, xs.at[z], own_sem.at[0]),
        pltpu.make_async_copy(c_in, cs.at[z], own_sem.at[1]),
    ]

    def weight(which, h):
        place = pl.ds(pl.multiple_of(h * cols, 128), cols)
        source = (wg_in.at[:, place], wu_in.at[:, place], wd_in.at[place, :])[which]
        return pltpu.make_async_copy(source, (wg, wu, wd)[which].at[h], w_sem.at[which, h])

    own[0].start()
    weight(0, 0).start()
    own[1].start()
    weight(1, 0).start()
    weight(2, 0).start()
    for h in range(1, halves):
        for which in range(3):
            weight(which, h).start()

    pl.semaphore_wait(barrier, bits + 2)

    below = {"mp": (z + n_mp - 1) % n_mp}

    def spread(which, p):
        there = (xs, cs)[which].at[(z + p - 1) % n_mp]
        return pltpu.make_async_remote_copy(
            src_ref=there, dst_ref=there,
            send_sem=tz_send.at[which, p - 1], recv_sem=tz_recv.at[which, p - 1],
            device_id=below, device_id_type=MESH,
        )

    def arrived(which, p):
        there = (xs, cs)[which].at[(z + p) % n_mp]
        return pltpu.make_async_remote_copy(
            src_ref=there, dst_ref=there,
            send_sem=tz_send.at[which, p - 1], recv_sem=tz_recv.at[which, p - 1],
            device_id=below, device_id_type=MESH,
        )

    for which in range(2):
        own[which].wait()
        spread(which, 1).start()

    def place_of(u):
        k = u // halves
        return k, u % halves, (z + k) % n_mp

    def keep_out(which, zz):
        return pltpu.make_async_copy(
            (xs, cs)[which].at[zz], (ax_ref, ac_ref)[which].at[zz], grid_sem.at[which, zz]
        )

    def put_out(i, h, zz, u):
        return pltpu.make_async_copy(
            gathered[i].at[zz, h],
            (hid_out, dg_out, du_out)[i].at[zz, :, :, pl.ds(pl.multiple_of(h * cols, 128), cols)],
            act_sem.at[u, i],
        )

    def rs(s, u, i):
        return pltpu.make_async_remote_copy(
            src_ref=snd[s].at[u % 2, i], dst_ref=rcv[s].at[u, i],
            send_sem=rs_send.at[s, u % 2, i], recv_sem=rs_recv.at[s, u, i],
            device_id={"dp": partner[s]}, device_id_type=MESH,
        )

    def ag(s, u, i, arriving=False):
        k, h, zz = place_of(u)
        size = pieces >> (s + 1)
        start = offset[s] + (1 - mine[s]) * size if arriving else offset[s + 1]
        there = gathered[i].at[zz, h, pl.ds(start, size)]
        return pltpu.make_async_remote_copy(
            src_ref=there, dst_ref=there,
            send_sem=ag_send.at[s, u % 2, i], recv_sem=ag_recv.at[s, u, i],
            device_id={"dp": partner[s]}, device_id_type=MESH,
        )

    def forward(i, u):
        k, h, zz = place_of(u)
        which = (0, 0, 1)[i]
        if i != 1:
            @pl.when((k > 0) & (h == 0))
            def _():
                arrived(which, k).wait_recv()

                @pl.when(k < n_mp - 1)
                def _():
                    spread(which, k + 1).start()

            @pl.when(h == 0)
            def _():
                keep_out(which, zz).start()

        @pl.when(u < halves)
        def _():
            weight(i, h).wait()

        if i == 0:
            total = contract(xs[zz], wg[h], 1, 0)
        elif i == 1:
            total = contract(xs[zz], wu[h], 1, 0)
        else:
            total = contract(cs[zz], wd[h], 1, 1)
        psum[i] = total.reshape(pieces, rows, cols)

        @pl.when(u >= 2)
        def _():
            rs(0, u - 2, i).wait_send()

        half = pieces // 2
        snd[0][u % 2, i] = psum[i, pl.ds((1 - mine[0]) * half, half)].astype(BF16)
        rs(0, u, i).start()

    def reduce(r, tensors, u):
        size = pieces >> r
        for i in tensors:
            rs(r - 1, u, i).wait_recv()
            if r == 1:
                old = psum.at[i, pl.ds(mine[0] * size, size)]
            else:
                old = kept[r - 2].at[u % 2, i]
            half = size // 2
            away, stay = (1 - mine[r]) * half, mine[r] * half

            @pl.when(u >= 2)
            def _():
                rs(r, u - 2, i).wait_send()

            new = rcv[r - 1].at[u, i]
            snd[r][u % 2, i] = (old[pl.ds(away, half)] + new[pl.ds(away, half)].astype(F32)).astype(BF16)
            rs(r, u, i).start()
            kept[r - 1][u % 2, i] = old[pl.ds(stay, half)] + new[pl.ds(stay, half)].astype(F32)

    def finish(u):
        k, h, zz = place_of(u)
        sums = []
        for i in range(3):
            rs(bits - 1, u, i).wait_recv()
            last = kept[bits - 2][u % 2, i] if bits > 1 else psum[i, pl.ds(mine[0], 1)]
            sums.append(last + rcv[bits - 1][u, i].astype(F32))
        gate, up, d_hidden = sums
        sig = 1.0 / (1.0 + jnp.exp(-gate))
        at = pl.ds(offset[bits], 1)
        hid[zz, h, at] = (gate * sig * up).astype(BF16)
        dg[zz, h, at] = (d_hidden * up * sig * (1.0 + gate * (1.0 - sig))).astype(BF16)
        du[zz, h, at] = (d_hidden * gate * sig).astype(BF16)
        for i in range(3):
            @pl.when(u >= 2)
            def _():
                ag(bits - 1, u - 2, i).wait_send()
            ag(bits - 1, u, i).start()

    def widen(a, u):
        for i in range(3):
            ag(a, u, i, arriving=True).wait_recv()

            @pl.when(u >= 2)
            def _():
                ag(a - 1, u - 2, i).wait_send()
            ag(a - 1, u, i).start()

    def backward(u):
        k, h, zz = place_of(u)
        other = jnp.minimum(k, 1)

        @pl.when(h == 0)
        def _():
            acc[other] = jnp.zeros(acc.shape[1:], F32)

        for i in range(3):
            ag(0, u, i, arriving=True).wait_recv()
            put_out(i, h, zz, u).start()
            left = gathered[i][zz, h].reshape(tall, cols)
            if i == 0:
                acc[other, 0] += contract(left, wd[h], 1, 0)
            elif i == 1:
                acc[other, 1] += contract(left, wg[h], 1, 1)
            else:
                acc[other, 1] += contract(left, wu[h], 1, 1)

        @pl.when((k > 0) & (k < n_mp - 1) & (h == halves - 1))
        def _():
            for i in range(2):
                total = passed(i, k)
                osend[k - 1, i] = total.astype(BF16)
                partial(i, k).start()

    def partial(i, k):
        return pltpu.make_async_remote_copy(
            src_ref=osend.at[k - 1, i], dst_ref=orecv.at[k, i],
            send_sem=o_send.at[k - 1, i], recv_sem=o_recv.at[k - 1, i],
            device_id=below, device_id_type=MESH,
        )

    def passed(i, k):
        @pl.when(k > 1)
        def _():
            partial(i, k - 1).wait_recv()
        return acc[1, i] + orecv[k - 1, i].astype(F32)

    run = {"gate": functools.partial(forward, 0), "up": functools.partial(forward, 1),
           "down": functools.partial(forward, 2)}
    for r in range(1, bits):
        run[f"rs{r}"] = functools.partial(reduce, r, range(3))
        run[f"ag{r}"] = functools.partial(widen, r)
    for i, name in enumerate(("gate", "up", "down")):
        run["rs1 " + name] = functools.partial(reduce, 1, (i,))
    run[f"rs{bits}"] = finish
    run["ag0"] = backward
    orecv[0] = jnp.zeros(orecv.shape[1:], BF16)
    order = tasks_of(bits)
    depth = max(lag for _, lag in order)

    def step(t, carry):
        for name, lag in order:
            u = t - lag

            @pl.when((u >= 0) & (u < units))
            def _():
                run[name](u)
        return carry

    lax.fori_loop(0, units + depth, step, 0)

    for i in range(2):
        last_ref[i] = passed(i, n_mp - 1).astype(BF16)
        mine_ref[i] = acc[0, i]

    for p in range(1, n_mp):
        for i in range(2):
            spread(i, p).wait_send()
            if p < n_mp - 1:
                partial(i, p).wait_send()
    first = max(units - 2, 0)
    for u in range(first, units):
        for s in range(bits):
            for i in range(3):
                rs(s, u, i).wait_send()
                ag(s, u, i).wait_send()

    def drain(u, carry):
        k, h, zz = place_of(u)
        for i in range(3):
            put_out(i, h, zz, u).wait()
        return carry

    lax.fori_loop(0, units, drain, 0)
    for zz in range(n_mp):
        for which in range(2):
            keep_out(which, zz).wait()


def gradients(x_ref, c_ref, h_ref, g_ref, u_ref, gg_ref, gu_ref, gd_ref, x_turned, h_turned, *, block):
    def body(*sums):
        sums = (sums[:2], sums[2:])
        used = 0

        @pl.when(pl.program_id(0) == 0)
        def _():
            x_turned[...] = x_ref[...].T
            for unit in range(2):
                for total in sums[unit]:
                    pltpu.matmul_pop(total)

        h_turned[...] = h_ref[...].T
        for left, right, out in (
            (x_turned, g_ref, gg_ref), (x_turned, u_ref, gu_ref), (h_turned, c_ref, gd_ref)
        ):
            (tall, depth), wide = left.shape, right.shape[1]
            for column in range(0, wide, 512):
                held = [(used + b) % 2 for b in range(tall // block)]
                used += tall // block
                for step in range(depth // 256):
                    deep = pl.ds(step * 256, 256)
                    for unit in range(2):
                        pltpu.matmul_push_rhs(
                            right[deep, pl.ds(column + unit * 256, 256)],
                            staging_register=step % 2, mxu_index=unit,
                        )
                    for b, which in enumerate(held):
                        for unit in range(2):
                            pltpu.matmul_acc_lhs(
                                sums[unit][which], left[pl.ds(b * block, block), deep],
                                load_staged_rhs=step % 2 if b == 0 else None,
                            )
                for b, which in enumerate(held):
                    for unit in range(2):
                        out[pl.ds(b * block, block), pl.ds(column + unit * 256, 256)] = (
                            pltpu.matmul_pop(sums[unit][which]).astype(BF16)
                        )

    pl.run_scoped(body, *[pltpu.ACC(unit)((block, 256), F32) for unit in range(2) for _ in range(2)])


def gradients_small(x_ref, c_ref, h_ref, g_ref, u_ref, gg_ref, gu_ref, gd_ref, turned):
    @pl.when(pl.program_id(0) == 0)
    def _():
        turned[...] = x_ref[...].T

    gd_ref[...] = contract(h_ref[...], c_ref[...], 0, 0).astype(BF16)
    gg_ref[...] = contract(turned[...], g_ref[...], 1, 0).astype(BF16)
    gu_ref[...] = contract(turned[...], u_ref[...], 1, 0).astype(BF16)


def weight_gradients(x, c, hidden, d_gate, d_up):
    (tall, width), inner = x.shape, hidden.shape[1]
    tile = next(t for t in (512, 256, 128) if inner % t == 0)
    explicit = tile == 512 and width % 512 == 0 and width <= 1024 and tall % 256 == 0
    scratch = [pltpu.VMEM((width, tall), BF16)]
    kernel = gradients_small
    if explicit:
        scratch.append(pltpu.VMEM((tile, tall), BF16))
        kernel = functools.partial(gradients, block=512)
    fixed = pl.BlockSpec((tall, width), lambda i: (0, 0), pipeline_mode=pl.Buffered(1))
    active = pl.BlockSpec((tall, tile), lambda i: (0, i))
    wide = pl.BlockSpec((width, tile), lambda i: (0, i))
    deep = pl.BlockSpec((tile, width), lambda i: (i, 0))
    return pl.pallas_call(
        kernel,
        grid=(inner // tile,),
        out_shape=(
            jax.ShapeDtypeStruct((width, inner), BF16), jax.ShapeDtypeStruct((width, inner), BF16),
            jax.ShapeDtypeStruct((inner, width), BF16),
        ),
        in_specs=[fixed, fixed, active, active, active],
        out_specs=(wide, wide, deep),
        scratch_shapes=scratch,
        compiler_params=pltpu.CompilerParams(vmem_limit_bytes=60 << 20),
        cost_estimate=pl.CostEstimate(
            flops=6 * tall * width * inner, transcendentals=0,
            bytes_accessed=6 * (tall + width) * inner + 4 * tall * width,
        ),
    )(x, c, hidden, d_gate, d_up)


def per_device(tokens, cotangent, gate_weight, up_weight, down_weight):
    n_dp, n_mp = lax.axis_size("dp"), lax.axis_size("mp")
    bits = n_dp.bit_length() - 1
    assert 1 << bits == n_dp and bits >= 2 and n_mp >= 3
    tall, width = tokens.shape
    inner = gate_weight.shape[1]
    halves = HALVES
    cols, units = inner // halves, n_mp * halves
    rows = tall // n_dp
    assert rows * n_dp == tall and cols * halves == inner

    vmem, any_ = pltpu.VMEM, pl.BlockSpec(memory_space=pl.ANY)
    in_vmem = pl.BlockSpec(memory_space=pltpu.VMEM)
    sizes = [n_dp >> (s + 1) for s in range(bits)]
    dma = pltpu.SemaphoreType.DMA
    scratch = [
        vmem((n_mp, tall, width), BF16), vmem((n_mp, tall, width), BF16),
        vmem((halves, width, cols), BF16), vmem((halves, width, cols), BF16),
        vmem((halves, cols, width), BF16),
    ]
    scratch += [vmem((n_mp, halves, n_dp, rows, cols), BF16)] * 3
    scratch += [
        vmem((3, n_dp, rows, cols), F32), vmem((2, 2, tall, width), F32),
        vmem((n_mp - 2, 2, tall, width), BF16), vmem((n_mp - 1, 2, tall, width), BF16),
    ]
    scratch += [vmem((2, 3, size, rows, cols), BF16) for size in sizes]
    scratch += [vmem((units, 3, size, rows, cols), BF16) for size in sizes]
    scratch += [vmem((2, 3, size, rows, cols), F32) for size in sizes[1:]]
    scratch += [
        dma((bits, 2, 3)), dma((bits, units, 3)), dma((bits, 2, 3)), dma((bits, units, 3)),
        dma((3, halves)), dma((2,)), dma((2, n_mp - 1)), dma((2, n_mp - 1)),
        dma((n_mp - 2, 2)), dma((n_mp - 2, 2)), dma((units, 3)), dma((2, n_mp)),
    ]
    small = [jax.ShapeDtypeStruct((2, tall, width), dtype) for dtype in (F32, BF16)]
    all_rows = jax.ShapeDtypeStruct((n_mp, tall, width), BF16)
    active = jax.ShapeDtypeStruct((n_mp, n_dp, rows, inner), BF16)
    mine, last, all_x, all_c, hidden, d_gate, d_up = pl.pallas_call(
        functools.partial(mixer, n_dp, n_mp, halves),
        out_shape=(*small, all_rows, all_rows, active, active, active),
        in_specs=[any_] * 5,
        out_specs=(in_vmem, in_vmem) + (any_,) * 5,
        scratch_shapes=scratch,
        compiler_params=pltpu.CompilerParams(
            collective_id=0, has_side_effects=True, vmem_limit_bytes=67043328
        ),
    )(tokens, cotangent, gate_weight, up_weight, down_weight)

    whole = n_mp * tall
    all_x, all_c = all_x.reshape(whole, width), all_c.reshape(whole, width)
    hidden, d_gate, d_up = (a.reshape(whole, inner) for a in (hidden, d_gate, d_up))
    come = lax.ppermute(last, "mp", [(i, (i - 1) % n_mp) for i in range(n_mp)])
    grad_gate, grad_up, grad_down = weight_gradients(all_x, all_c, hidden, d_gate, d_up)
    output = (mine[0] + come[0].astype(F32)).astype(BF16)
    grad_input = (mine[1] + come[1].astype(F32)).astype(BF16)
    return (output, grad_input, grad_gate, grad_up, grad_down)


def solution(mesh):
    placed = (P("mp", "dp"), P("mp", "dp"), P("dp", "mp"), P("dp", "mp"), P("mp", "dp"))
    return jax.shard_map(
        per_device,
        mesh=mesh,
        in_specs=placed,
        out_specs=(P("mp", "dp"), P("mp", "dp"), P("dp", "mp"), P("dp", "mp"), P("mp", "dp")),
        check_vma=False,
    )
```

```python
import functools

import jax
import jax.numpy as jnp
from jax import lax
from jax.experimental import pallas as pl
from jax.experimental.pallas import tpu as pltpu
from jax.sharding import PartitionSpec as P

F32, BF16 = jnp.float32, jnp.bfloat16
MESH = pl.DeviceIdType.MESH

HALVES = 2
ORDER = (
    ("gate", 0),
    ("up", 0),
    ("rs1 gate", 0),
    ("down", 0),
    ("rs1 up", 0),
    ("rs1 down", 0),
    ("rs3", 2),
    ("rs2", 1),
    ("ag2", 3),
    ("ag1", 4),
    ("ag0", 4),
)


def contract(left, right, left_dim, right_dim):
    return lax.dot_general(
        left, right, (((left_dim,), (right_dim,)), ((), ())), preferred_element_type=F32
    )


def tasks_of(bits):
    if bits == 3:
        return ORDER
    order = [("gate", 0), ("up", 0), ("down", 0), ("rs1", 0)]
    order += [(f"rs{r}", r - 1) for r in range(2, bits + 1)]
    order += [(f"ag{a}", 2 * bits - 1 - a) for a in range(bits - 1, -1, -1)]
    return tuple(order)


def mixer(
    n_dp, n_mp, halves,
    x_in, c_in, wg_in, wu_in, wd_in,
    mine_ref, last_ref, ax_ref, ac_ref, hid_out, dg_out, du_out,
    xs, cs, wg, wu, wd, hid, dg, du, psum, acc, osend, orecv, *rest,
):
    bits = n_dp.bit_length() - 1
    snd, rcv, kept = rest[:bits], rest[bits:2 * bits], rest[2 * bits:3 * bits - 1]
    (rs_send, rs_recv, ag_send, ag_recv, w_sem, own_sem, tz_send, tz_recv,
     o_send, o_recv, act_sem, grid_sem) = rest[3 * bits - 1:]
    units = n_mp * halves
    pieces, rows, cols = psum.shape[1:]
    tall = pieces * rows
    gathered = (hid, dg, du)

    me, z = lax.axis_index("dp"), lax.axis_index("mp")
    parity = me % 2
    even = [0] + list(range(1, bits))
    odd = [0] + list(range(bits - 1, 0, -1))
    partner, offset, mine = [], [0], []
    for s in range(bits):
        width = (1 << even[s]) * (1 - parity) + (1 << odd[s]) * parity
        bit = (me // width) % 2
        mine.append(bit)
        partner.append(me + width * (1 - 2 * bit))
        offset.append(offset[-1] + bit * (pieces >> (s + 1)))

    barrier = pltpu.get_barrier_semaphore()
    for s in range(bits):
        pl.semaphore_signal(barrier, inc=1, device_id={"dp": partner[s]}, device_id_type=MESH)
    for k in (1, n_mp - 1):
        pl.semaphore_signal(barrier, inc=1, device_id={"mp": (z + k) % n_mp}, device_id_type=MESH)

    own = [
        pltpu.make_async_copy(x_in, xs.at[z], own_sem.at[0]),
        pltpu.make_async_copy(c_in, cs.at[z], own_sem.at[1]),
    ]

    def weight(which, h):
        place = pl.ds(pl.multiple_of(h * cols, 128), cols)
        source = (wg_in.at[:, place], wu_in.at[:, place], wd_in.at[place, :])[which]
        return pltpu.make_async_copy(source, (wg, wu, wd)[which].at[h], w_sem.at[which, h])

    own[0].start()
    weight(0, 0).start()
    own[1].start()
    weight(1, 0).start()

    pl.semaphore_wait(barrier, bits + 2)

    below = {"mp": (z + n_mp - 1) % n_mp}

    def spread(which, p):
        there = (xs, cs)[which].at[(z + p - 1) % n_mp]
        return pltpu.make_async_remote_copy(
            src_ref=there, dst_ref=there,
            send_sem=tz_send.at[which, p - 1], recv_sem=tz_recv.at[which, p - 1],
            device_id=below, device_id_type=MESH,
        )

    def arrived(which, p):
        there = (xs, cs)[which].at[(z + p) % n_mp]
        return pltpu.make_async_remote_copy(
            src_ref=there, dst_ref=there,
            send_sem=tz_send.at[which, p - 1], recv_sem=tz_recv.at[which, p - 1],
            device_id=below, device_id_type=MESH,
        )

    for which in range(2):
        own[which].wait()
        spread(which, 1).start()

    def place_of(u):
        k = u // halves
        return k, u % halves, (z + k) % n_mp

    def keep_out(which, zz):
        return pltpu.make_async_copy(
            (xs, cs)[which].at[zz], (ax_ref, ac_ref)[which].at[zz], grid_sem.at[which, zz]
        )

    def put_out(i, h, zz, u):
        return pltpu.make_async_copy(
            gathered[i].at[zz, h],
            (hid_out, dg_out, du_out)[i].at[zz, :, :, pl.ds(pl.multiple_of(h * cols, 128), cols)],
            act_sem.at[u, i],
        )

    def rs(s, u, i):
        return pltpu.make_async_remote_copy(
            src_ref=snd[s].at[u % 2, i], dst_ref=rcv[s].at[u, i],
            send_sem=rs_send.at[s, u % 2, i], recv_sem=rs_recv.at[s, u, i],
            device_id={"dp": partner[s]}, device_id_type=MESH,
        )

    def ag(s, u, i, arriving=False):
        k, h, zz = place_of(u)
        size = pieces >> (s + 1)
        start = offset[s] + (1 - mine[s]) * size if arriving else offset[s + 1]
        there = gathered[i].at[zz, h, pl.ds(start, size)]
        return pltpu.make_async_remote_copy(
            src_ref=there, dst_ref=there,
            send_sem=ag_send.at[s, u % 2, i], recv_sem=ag_recv.at[s, u, i],
            device_id={"dp": partner[s]}, device_id_type=MESH,
        )

    def forward(i, u):
        k, h, zz = place_of(u)
        which = (0, 0, 1)[i]
        if i != 1:
            @pl.when((k > 0) & (h == 0))
            def _():
                arrived(which, k).wait_recv()

                @pl.when(k < n_mp - 1)
                def _():
                    spread(which, k + 1).start()

            @pl.when(h == 0)
            def _():
                keep_out(which, zz).start()

        @pl.when(u < halves)
        def _():
            weight(i, h).wait()
            later = 0 if i == 0 else 1

            @pl.when(h + later < halves)
            def _():
                weight((i + 2) % 3, h + later).start()

        if i == 0:
            total = contract(xs[zz], wg[h], 1, 0)
        elif i == 1:
            total = contract(xs[zz], wu[h], 1, 0)
        else:
            total = contract(cs[zz], wd[h], 1, 1)
        psum[i] = total.reshape(pieces, rows, cols)

        @pl.when(u >= 2)
        def _():
            rs(0, u - 2, i).wait_send()

        half = pieces // 2
        snd[0][u % 2, i] = psum[i, pl.ds((1 - mine[0]) * half, half)].astype(BF16)
        rs(0, u, i).start()

    def reduce(r, tensors, u):
        size = pieces >> r
        for i in tensors:
            rs(r - 1, u, i).wait_recv()
            if r == 1:
                old = psum.at[i, pl.ds(mine[0] * size, size)]
            else:
                old = kept[r - 2].at[u % 2, i]
            half = size // 2
            away, stay = (1 - mine[r]) * half, mine[r] * half

            @pl.when(u >= 2)
            def _():
                rs(r, u - 2, i).wait_send()

            new = rcv[r - 1].at[u, i]
            snd[r][u % 2, i] = (old[pl.ds(away, half)] + new[pl.ds(away, half)].astype(F32)).astype(BF16)
            rs(r, u, i).start()
            kept[r - 1][u % 2, i] = old[pl.ds(stay, half)] + new[pl.ds(stay, half)].astype(F32)

    def finish(u):
        k, h, zz = place_of(u)
        sums = []
        for i in range(3):
            rs(bits - 1, u, i).wait_recv()
            last = kept[bits - 2][u % 2, i] if bits > 1 else psum[i, pl.ds(mine[0], 1)]
            sums.append(last + rcv[bits - 1][u, i].astype(F32))
        gate, up, d_hidden = sums
        sig = 1.0 / (1.0 + jnp.exp(-gate))
        at = pl.ds(offset[bits], 1)
        hid[zz, h, at] = (gate * sig * up).astype(BF16)
        dg[zz, h, at] = (d_hidden * up * sig * (1.0 + gate * (1.0 - sig))).astype(BF16)
        du[zz, h, at] = (d_hidden * gate * sig).astype(BF16)
        for i in range(3):
            @pl.when(u >= 2)
            def _():
                ag(bits - 1, u - 2, i).wait_send()
            ag(bits - 1, u, i).start()

    def widen(a, u):
        for i in range(3):
            ag(a, u, i, arriving=True).wait_recv()

            @pl.when(u >= 2)
            def _():
                ag(a - 1, u - 2, i).wait_send()
            ag(a - 1, u, i).start()

    def backward(u):
        k, h, zz = place_of(u)
        other = jnp.minimum(k, 1)

        @pl.when(h == 0)
        def _():
            acc[other] = jnp.zeros(acc.shape[1:], F32)

        for i in range(3):
            ag(0, u, i, arriving=True).wait_recv()
            put_out(i, h, zz, u).start()
            left = gathered[i][zz, h].reshape(tall, cols)
            if i == 0:
                acc[other, 0] += contract(left, wd[h], 1, 0)
            elif i == 1:
                acc[other, 1] += contract(left, wg[h], 1, 1)
            else:
                acc[other, 1] += contract(left, wu[h], 1, 1)

        @pl.when((k > 0) & (k < n_mp - 1) & (h == halves - 1))
        def _():
            for i in range(2):
                total = passed(i, k)
                osend[k - 1, i] = total.astype(BF16)
                partial(i, k).start()

    def partial(i, k):
        return pltpu.make_async_remote_copy(
            src_ref=osend.at[k - 1, i], dst_ref=orecv.at[k, i],
            send_sem=o_send.at[k - 1, i], recv_sem=o_recv.at[k - 1, i],
            device_id=below, device_id_type=MESH,
        )

    def passed(i, k):
        @pl.when(k > 1)
        def _():
            partial(i, k - 1).wait_recv()
        return acc[1, i] + orecv[k - 1, i].astype(F32)

    run = {"gate": functools.partial(forward, 0), "up": functools.partial(forward, 1),
           "down": functools.partial(forward, 2)}
    for r in range(1, bits):
        run[f"rs{r}"] = functools.partial(reduce, r, range(3))
        run[f"ag{r}"] = functools.partial(widen, r)
    for i, name in enumerate(("gate", "up", "down")):
        run["rs1 " + name] = functools.partial(reduce, 1, (i,))
    run[f"rs{bits}"] = finish
    run["ag0"] = backward
    orecv[0] = jnp.zeros(orecv.shape[1:], BF16)
    order = tasks_of(bits)
    depth = max(lag for _, lag in order)

    def step(t, carry):
        for name, lag in order:
            u = t - lag

            @pl.when((u >= 0) & (u < units))
            def _():
                run[name](u)
        return carry

    lax.fori_loop(0, units + depth, step, 0)

    for i in range(2):
        last_ref[i] = passed(i, n_mp - 1).astype(BF16)
        mine_ref[i] = acc[0, i]

    for p in range(1, n_mp):
        for i in range(2):
            spread(i, p).wait_send()
            if p < n_mp - 1:
                partial(i, p).wait_send()
    first = max(units - 2, 0)
    for u in range(first, units):
        for s in range(bits):
            for i in range(3):
                rs(s, u, i).wait_send()
                ag(s, u, i).wait_send()

    def drain(u, carry):
        k, h, zz = place_of(u)
        for i in range(3):
            put_out(i, h, zz, u).wait()
        return carry

    lax.fori_loop(0, units, drain, 0)
    for zz in range(n_mp):
        for which in range(2):
            keep_out(which, zz).wait()


def gradients(x_ref, c_ref, h_ref, g_ref, u_ref, gg_ref, gu_ref, gd_ref, x_turned, h_turned, *, block):
    def body(*sums):
        sums = (sums[:2], sums[2:])
        used = 0

        @pl.when(pl.program_id(0) == 0)
        def _():
            x_turned[...] = x_ref[...].T
            for unit in range(2):
                for total in sums[unit]:
                    pltpu.matmul_pop(total)

        h_turned[...] = h_ref[...].T
        for left, right, out in (
            (x_turned, g_ref, gg_ref), (x_turned, u_ref, gu_ref), (h_turned, c_ref, gd_ref)
        ):
            (tall, depth), wide = left.shape, right.shape[1]
            for column in range(0, wide, 512):
                held = [(used + b) % 2 for b in range(tall // block)]
                used += tall // block
                for step in range(depth // 256):
                    deep = pl.ds(step * 256, 256)
                    for unit in range(2):
                        pltpu.matmul_push_rhs(
                            right[deep, pl.ds(column + unit * 256, 256)],
                            staging_register=step % 2, mxu_index=unit,
                        )
                    for b, which in enumerate(held):
                        for unit in range(2):
                            pltpu.matmul_acc_lhs(
                                sums[unit][which], left[pl.ds(b * block, block), deep],
                                load_staged_rhs=step % 2 if b == 0 else None,
                            )
                for b, which in enumerate(held):
                    for unit in range(2):
                        out[pl.ds(b * block, block), pl.ds(column + unit * 256, 256)] = (
                            pltpu.matmul_pop(sums[unit][which]).astype(BF16)
                        )

    pl.run_scoped(body, *[pltpu.ACC(unit)((block, 256), F32) for unit in range(2) for _ in range(2)])


def gradients_small(x_ref, c_ref, h_ref, g_ref, u_ref, gg_ref, gu_ref, gd_ref, turned):
    @pl.when(pl.program_id(0) == 0)
    def _():
        turned[...] = x_ref[...].T

    gd_ref[...] = contract(h_ref[...], c_ref[...], 0, 0).astype(BF16)
    gg_ref[...] = contract(turned[...], g_ref[...], 1, 0).astype(BF16)
    gu_ref[...] = contract(turned[...], u_ref[...], 1, 0).astype(BF16)


def weight_gradients(x, c, hidden, d_gate, d_up):
    (tall, width), inner = x.shape, hidden.shape[1]
    tile = next(t for t in (512, 256, 128) if inner % t == 0)
    explicit = tile == 512 and width % 512 == 0 and width <= 1024 and tall % 256 == 0
    scratch = [pltpu.VMEM((width, tall), BF16)]
    kernel = gradients_small
    if explicit:
        scratch.append(pltpu.VMEM((tile, tall), BF16))
        kernel = functools.partial(gradients, block=512)
    fixed = pl.BlockSpec((tall, width), lambda i: (0, 0), pipeline_mode=pl.Buffered(1))
    active = pl.BlockSpec((tall, tile), lambda i: (0, i))
    wide = pl.BlockSpec((width, tile), lambda i: (0, i))
    deep = pl.BlockSpec((tile, width), lambda i: (i, 0))
    return pl.pallas_call(
        kernel,
        grid=(inner // tile,),
        out_shape=(
            jax.ShapeDtypeStruct((width, inner), BF16), jax.ShapeDtypeStruct((width, inner), BF16),
            jax.ShapeDtypeStruct((inner, width), BF16),
        ),
        in_specs=[fixed, fixed, active, active, active],
        out_specs=(wide, wide, deep),
        scratch_shapes=scratch,
        compiler_params=pltpu.CompilerParams(vmem_limit_bytes=60 << 20),
        cost_estimate=pl.CostEstimate(
            flops=6 * tall * width * inner, transcendentals=0,
            bytes_accessed=6 * (tall + width) * inner + 4 * tall * width,
        ),
    )(x, c, hidden, d_gate, d_up)


def per_device(tokens, cotangent, gate_weight, up_weight, down_weight):
    n_dp, n_mp = lax.axis_size("dp"), lax.axis_size("mp")
    bits = n_dp.bit_length() - 1
    assert 1 << bits == n_dp and bits >= 2 and n_mp >= 3
    tall, width = tokens.shape
    inner = gate_weight.shape[1]
    halves = HALVES
    cols, units = inner // halves, n_mp * halves
    rows = tall // n_dp
    assert rows * n_dp == tall and cols * halves == inner

    vmem, any_ = pltpu.VMEM, pl.BlockSpec(memory_space=pl.ANY)
    in_vmem = pl.BlockSpec(memory_space=pltpu.VMEM)
    sizes = [n_dp >> (s + 1) for s in range(bits)]
    dma = pltpu.SemaphoreType.DMA
    scratch = [
        vmem((n_mp, tall, width), BF16), vmem((n_mp, tall, width), BF16),
        vmem((halves, width, cols), BF16), vmem((halves, width, cols), BF16),
        vmem((halves, cols, width), BF16),
    ]
    scratch += [vmem((n_mp, halves, n_dp, rows, cols), BF16)] * 3
    scratch += [
        vmem((3, n_dp, rows, cols), F32), vmem((2, 2, tall, width), F32),
        vmem((n_mp - 2, 2, tall, width), BF16), vmem((n_mp - 1, 2, tall, width), BF16),
    ]
    scratch += [vmem((2, 3, size, rows, cols), BF16) for size in sizes]
    scratch += [vmem((units, 3, size, rows, cols), BF16) for size in sizes]
    scratch += [vmem((2, 3, size, rows, cols), F32) for size in sizes[1:]]
    scratch += [
        dma((bits, 2, 3)), dma((bits, units, 3)), dma((bits, 2, 3)), dma((bits, units, 3)),
        dma((3, halves)), dma((2,)), dma((2, n_mp - 1)), dma((2, n_mp - 1)),
        dma((n_mp - 2, 2)), dma((n_mp - 2, 2)), dma((units, 3)), dma((2, n_mp)),
    ]
    small = [jax.ShapeDtypeStruct((2, tall, width), dtype) for dtype in (F32, BF16)]
    all_rows = jax.ShapeDtypeStruct((n_mp, tall, width), BF16)
    active = jax.ShapeDtypeStruct((n_mp, n_dp, rows, inner), BF16)
    mine, last, all_x, all_c, hidden, d_gate, d_up = pl.pallas_call(
        functools.partial(mixer, n_dp, n_mp, halves),
        out_shape=(*small, all_rows, all_rows, active, active, active),
        in_specs=[any_] * 5,
        out_specs=(in_vmem, in_vmem) + (any_,) * 5,
        scratch_shapes=scratch,
        compiler_params=pltpu.CompilerParams(
            collective_id=0, has_side_effects=True, vmem_limit_bytes=67043328
        ),
    )(tokens, cotangent, gate_weight, up_weight, down_weight)

    whole = n_mp * tall
    all_x, all_c = all_x.reshape(whole, width), all_c.reshape(whole, width)
    hidden, d_gate, d_up = (a.reshape(whole, inner) for a in (hidden, d_gate, d_up))
    come = lax.ppermute(last, "mp", [(i, (i - 1) % n_mp) for i in range(n_mp)])
    grad_gate, grad_up, grad_down = weight_gradients(all_x, all_c, hidden, d_gate, d_up)
    output = (mine[0] + come[0].astype(F32)).astype(BF16)
    grad_input = (mine[1] + come[1].astype(F32)).astype(BF16)
    return (output, grad_input, grad_gate, grad_up, grad_down)


def solution(mesh):
    placed = (P("mp", "dp"), P("mp", "dp"), P("dp", "mp"), P("dp", "mp"), P("mp", "dp"))
    return jax.shard_map(
        per_device,
        mesh=mesh,
        in_specs=placed,
        out_specs=(P("mp", "dp"), P("mp", "dp"), P("dp", "mp"), P("dp", "mp"), P("mp", "dp")),
        check_vma=False,
    )
```
